32 devices in a mesh: chan: 8 (over z, y), beam: 4 (over x, core).
Axes of the slice: x: 2, y: 2, z: 4, core: 2. Of those that a mesh axis runs over, the one named last changes fastest.
Arguments:
- signals: bfloat16 [2048, 8192], P('chan', 'beam'), may hold values from -6 to 6
- weights: bfloat16 [3, 2, 512, 2048], P(None, None, 'beam', 'chan'), may hold values from -0.125 to 0.125
- bin_group: int32 [256], replicated, may hold values from 0 to 2
Outputs:
- formed: float32 [256, 2, 512], P('chan', None, 'beam')
The draws below stay inside these ranges and needn't reach their ends.
All inputs are finite; a program needn't handle non-finite values.
Results may differ from the reference program's by a relative error of at most 0.0042.
Values may be sent and summed in bfloat16 or wider, within the bound.
A program may use at most 64 MiB of HBM per device.

```python
import math
import jax
import jax.numpy as jnp

SAMPLES = 8192
BEAMS = 512
GROUPS = 3
CHANNELS = 2048
BINS = 256


def place_ends(array, stream_key, smallest, top_value):
    longest = array.shape.index(max(array.shape))
    spots = []
    for shift in (0, 1):
        where = [jax.random.randint(jax.random.fold_in(stream_key, axis), (), 0, length) for axis, length in enumerate(array.shape)]
        where[longest] = (where[longest] + shift) % array.shape[longest]
        spots.append(tuple(where))
    return array.at[spots[0]].set(smallest).at[spots[1]].set(top_value)


def steps_of(rng, extent, shards, smallest, top_value):
    def one(position, blocks):
        heights = jax.random.uniform(jax.random.fold_in(jax.random.fold_in(rng, 6), position), (blocks,), jnp.float32, smallest / len(shards), top_value / len(shards))
        return jnp.repeat(jnp.exp(heights), extent[position] // blocks).reshape((-1,) + (1,) * (len(extent) - position - 1))

    level = one(*shards[0])
    for cut in shards[1:]:
        level = level * one(*cut)
    return level


def gaussian(stream_key, extent, deviation, bound, shards=(), held_as=jnp.bfloat16):
    array = deviation * jax.random.normal(stream_key, extent, jnp.float32)
    if shards:
        array = array * steps_of(stream_key, extent, shards, -0.22, 0.18)
    return jnp.clip(array, -bound, bound).astype(held_as)


def setup_inputs(seed: int = 0) -> dict:
    keys = jax.random.split(jax.random.key(seed), 4)
    return {
        "signals": gaussian(keys[0], (CHANNELS, SAMPLES), 1.0, 6.0, ((0, 8), (1, 4))),
        "weights": gaussian(keys[1], (GROUPS, 2, BEAMS, CHANNELS), CHANNELS ** -0.5, 0.125, ((2, 4), (3, 8))),
        "bin_group": place_ends(jax.random.randint(keys[2], (BINS,), 0, GROUPS), jax.random.fold_in(keys[2], 1), 0, GROUPS - 1).astype(jnp.int32),
    }


def reference(signals, weights, bin_group):
    frequency = jnp.arange(1, BINS + 1, dtype=jnp.int32)
    sample_index = jnp.arange(SAMPLES, dtype=jnp.int32)
    phases = frequency[:, None] * sample_index[None, :] % SAMPLES
    angles = 2.0 * math.pi / SAMPLES * phases.astype(jnp.float32)
    twiddle = jnp.stack([jnp.cos(angles), -jnp.sin(angles)], 1).astype(jnp.bfloat16)
    summed = jnp.dot(twiddle.reshape(2 * BINS, SAMPLES), signals.T, preferred_element_type=jnp.float32)
    spectrum = (summed * (1.0 / math.sqrt(SAMPLES))).astype(jnp.bfloat16).reshape(BINS, 2, CHANNELS)
    spec_real = spectrum[:, 0]
    spec_imag = spectrum[:, 1]
    formed = jnp.zeros((BINS, 2, BEAMS), jnp.float32)
    for group_id in range(GROUPS):
        w_real = weights[group_id, 0].T
        w_imag = weights[group_id, 1].T
        real_real = jnp.dot(spec_real, w_real, preferred_element_type=jnp.float32)
        imag_imag = jnp.dot(spec_imag, w_imag, preferred_element_type=jnp.float32)
        imag_real = jnp.dot(spec_imag, w_real, preferred_element_type=jnp.float32)
        real_imag = jnp.dot(spec_real, w_imag, preferred_element_type=jnp.float32)
        chosen = (bin_group == group_id).astype(jnp.float32)[:, None, None]
        formed = formed + chosen * jnp.stack([real_real - imag_imag, imag_real + real_imag], 1)
    return formed
```

```python
import functools
import math

import jax
import jax.numpy as jnp
from jax import lax
from jax.experimental import pallas as pl
from jax.experimental.pallas import tpu as pltpu
from jax.sharding import PartitionSpec as P

MESH = pl.DeviceIdType.MESH
LANES = 128
ROWS = 16
NT = (((1,), (1,)), ((), ()))


def cos_sin(phase, period):
    quarter = period // 4
    turn = (phase + quarter // 2) // quarter
    angle = (phase - turn * quarter).astype(jnp.float32) * (2.0 * math.pi / period)
    square = angle * angle
    sine = angle * (1 + square * (-1 / 6 + square * (1 / 120 + square * (-1 / 5040 + square / 362880))))
    cosine = 1 + square * (
        -1 / 2 + square * (1 / 24 + square * (-1 / 720 + square * (1 / 40320 - square / 3628800)))
    )
    turn = turn & 3
    swap = (turn & 1) == 1
    first = jnp.where(swap, sine, cosine)
    second = jnp.where(swap, cosine, sine)
    cos_value = jnp.where((turn == 1) | (turn == 2), -first, first)
    sin_value = jnp.where(turn >= 2, -second, second)
    return cos_value, sin_value


def kernel(
    n_chan, n_beam,
    signals_hbm, weights_hbm, group_ref, out_ref,
    signals, weights, twiddle, part, from_pair, from_far, spectrum, group_rows, formed, arrived,
    load_sem, pair_send, pair_recv, far_send, far_recv, spec_send, spec_recv, form_send, form_recv,
):
    chan, beam = lax.axis_index("chan"), lax.axis_index("beam")
    core = lax.rem(beam, 2)
    far_count = n_beam // 2 - 1
    partner = beam + 1 - 2 * core
    fars = [lax.rem(beam + 2 * (s + 1), n_beam) for s in range(far_count)]
    chans = [lax.rem(chan + s + 1, n_chan) for s in range(n_chan - 1)]

    barrier = pltpu.get_barrier_semaphore()
    for other in [partner] + fars:
        pl.semaphore_signal(barrier, inc=1, device_id={"beam": other}, device_id_type=MESH)
    for other in chans:
        pl.semaphore_signal(barrier, inc=1, device_id={"chan": other}, device_id_type=MESH)

    load_signals = pltpu.make_async_copy(signals_hbm, signals, load_sem.at[0])
    load_weights = pltpu.make_async_copy(weights_hbm, weights, load_sem.at[1])
    load_signals.start()
    load_weights.start()

    half, samples = part.shape[2], signals.shape[1]
    block = twiddle.shape[1]
    total = samples * n_beam
    bins = half * 2
    bin_dev = bins // n_chan
    chunks = half // bin_dev
    sets, _, beams, channels = weights.shape
    scale = 1.0 / math.sqrt(total)

    def transform(which, wait):
        def one(step, carry):
            first_bin = which * half + step * block

            def rows(row, carry):
                base = pl.multiple_of(row * ROWS, ROWS)
                frequency = first_bin + base + 1 + lax.broadcasted_iota(jnp.int32, (ROWS, LANES), 0)
                lane = lax.broadcasted_iota(jnp.int32, (ROWS, LANES), 1)
                cos_low, sin_low = cos_sin((frequency * lane) & (total - 1), total)
                high = beam * samples + lane * LANES
                cos_high, sin_high = cos_sin((frequency * high) & (total - 1), total)
                for a in range(samples // LANES):
                    ca = jnp.broadcast_to(cos_high[:, a : a + 1], (ROWS, LANES))
                    sa = jnp.broadcast_to(sin_high[:, a : a + 1], (ROWS, LANES))
                    columns = pl.ds(a * LANES, LANES)
                    twiddle[0, pl.ds(base, ROWS), columns] = (ca * cos_low - sa * sin_low).astype(jnp.bfloat16)
                    twiddle[1, pl.ds(base, ROWS), columns] = (-(sa * cos_low + ca * sin_low)).astype(jnp.bfloat16)
                return carry

            lax.fori_loop(0, block // ROWS, rows, 0)
            if wait:
                load_signals.wait()
            summed = lax.dot_general(
                twiddle[...].reshape(2 * block, samples), signals[...], NT, preferred_element_type=jnp.float32
            )
            at = pl.ds(pl.multiple_of(step * block, block), block)
            part[which, 0, at] = summed[:block]
            part[which, 1, at] = summed[block:]
            return carry

        if half == block:
            one(0, 0)
        else:
            lax.fori_loop(0, half // block, one, 0)

    if half != block:
        load_signals.wait()
    transform(1 - core, half == block)

    pl.semaphore_wait(barrier, n_beam // 2 + n_chan - 1)
    to_pair = pltpu.make_async_remote_copy(
        src_ref=part.at[1 - core], dst_ref=from_pair, send_sem=pair_send, recv_sem=pair_recv,
        device_id={"beam": partner}, device_id_type=MESH,
    )
    to_pair.start()
    transform(core, False)

    group = jnp.broadcast_to(group_ref[...].astype(jnp.float32), (LANES, bins))
    group_rows[...] = group.T

    to_pair.wait_recv()

    def order(step):
        return lax.rem(chan + 1 + step, chunks)

    def rows_of(chunk):
        return pl.ds(pl.multiple_of(chunk * bin_dev, bin_dev), bin_dev)

    def far_copy(chunk, s):
        return pltpu.make_async_remote_copy(
            src_ref=part.at[core, :, rows_of(chunk)], dst_ref=from_far.at[s, :, rows_of(chunk)],
            send_sem=far_send.at[s, chunk], recv_sem=far_recv.at[s, chunk],
            device_id={"beam": fars[s]}, device_id_type=MESH,
        )

    def spec_copy(which, chunk):
        return pltpu.make_async_remote_copy(
            src_ref=spectrum.at[which, :, rows_of(chunk)], dst_ref=spectrum.at[which, :, rows_of(chunk)],
            send_sem=spec_send.at[chunk], recv_sem=spec_recv.at[chunk],
            device_id={"beam": partner}, device_id_type=MESH,
        )

    def form_copy(source, target):
        return pltpu.make_async_remote_copy(
            src_ref=formed.at[target], dst_ref=arrived.at[source],
            send_sem=form_send.at[target], recv_sem=form_recv.at[source],
            device_id={"chan": target}, device_id_type=MESH,
        )

    for step in range(chunks):
        chunk = order(step)
        at = rows_of(chunk)
        part[core, :, at] = part[core, :, at] + from_pair[:, at]
        for s in range(far_count):
            far_copy(chunk, s).start()

    load_weights.wait()

    def form(which, chunk):
        at = rows_of(chunk)
        target = which * chunks + chunk
        spec = spectrum[which, :, at].reshape(2 * bin_dev, channels)
        products = lax.dot_general(
            spec, weights[...].reshape(sets * 2 * beams, channels), NT, preferred_element_type=jnp.float32
        )
        ids = group_rows[pl.ds(pl.multiple_of(target * bin_dev, bin_dev), bin_dev), :]
        real = imag = jnp.zeros((bin_dev, beams), jnp.float32)
        for g in range(sets):
            left = slice(2 * g * beams, (2 * g + 1) * beams)
            right = slice((2 * g + 1) * beams, (2 * g + 2) * beams)
            chosen = ids[:, :1] == g
            real = jnp.where(chosen, products[:bin_dev, left] - products[bin_dev:, right], real)
            imag = jnp.where(chosen, products[bin_dev:, left] + products[:bin_dev, right], imag)
        formed[target, 0] = real
        formed[target, 1] = imag

        @pl.when(target != chan)
        def _():
            form_copy(chan, target).start()

    def far_sum(chunk):
        at = rows_of(chunk)
        value = part[core, :, at]
        for s in range(far_count):
            far_copy(chunk, s).wait_recv()
            value = value + from_far[s, :, at]
        spectrum[core, :, at] = (value * scale).astype(jnp.bfloat16)
        spec_copy(core, chunk).start()

    for step in range(chunks):
        chunk = order(step)
        far_sum(chunk)
        form(core, chunk)
        if step:
            before = order(step - 1)
            spec_copy(1 - core, before).wait_recv()
            form(1 - core, before)
    last = order(chunks - 1)
    spec_copy(1 - core, last).wait_recv()
    form(1 - core, last)

    value = formed[chan]
    for other in reversed(chans):
        form_copy(other, other).wait_recv()
        value = value + arrived[other]
    out_ref[...] = value

    to_pair.wait_send()
    for chunk in range(chunks):
        for s in range(far_count):
            far_copy(chunk, s).wait_send()
        spec_copy(core, chunk).wait_send()
    for other in chans:
        form_copy(chan, other).wait_send()


def shards(n_chan, n_beam, signals, weights, bin_group):
    channels, samples = signals.shape
    sets, _, beams, _ = weights.shape
    bins = bin_group.shape[0]
    half, bin_dev = bins // 2, bins // n_chan
    chunks = half // bin_dev
    fars = n_beam // 2 - 1
    block = min(half, 128)
    dma = pltpu.SemaphoreType.DMA
    out = pl.pallas_call(
        functools.partial(kernel, n_chan, n_beam),
        out_shape=jax.ShapeDtypeStruct((2, bin_dev, beams), jnp.float32),
        in_specs=[
            pl.BlockSpec(memory_space=pl.ANY),
            pl.BlockSpec(memory_space=pl.ANY),
            pl.BlockSpec(memory_space=pltpu.VMEM),
        ],
        out_specs=pl.BlockSpec(memory_space=pltpu.VMEM),
        scratch_shapes=[
            pltpu.VMEM(signals.shape, signals.dtype),
            pltpu.VMEM(weights.shape, weights.dtype),
            pltpu.VMEM((2, block, samples), jnp.bfloat16),
            pltpu.VMEM((2, 2, half, channels), jnp.float32),
            pltpu.VMEM((2, half, channels), jnp.float32),
            pltpu.VMEM((fars, 2, half, channels), jnp.float32),
            pltpu.VMEM((2, 2, half, channels), jnp.bfloat16),
            pltpu.VMEM((bins, LANES), jnp.float32),
            pltpu.VMEM((n_chan, 2, bin_dev, beams), jnp.float32),
            pltpu.VMEM((n_chan, 2, bin_dev, beams), jnp.float32),
            dma((2,)), dma, dma, dma((fars, chunks)), dma((fars, chunks)),
            dma((chunks,)), dma((chunks,)), dma((n_chan,)), dma((n_chan,)),
        ],
        compiler_params=pltpu.CompilerParams(
            collective_id=0, has_side_effects=True, vmem_limit_bytes=60 * 1024 * 1024
        ),
        name="beamform",
    )(signals, weights, bin_group.reshape(1, bins))
    return jnp.swapaxes(out, 0, 1)


def solution(mesh):
    in_specs = (P("chan", "beam"), P(None, None, "beam", "chan"), P())
    out_specs = P("chan", None, "beam")
    body = functools.partial(shards, mesh.shape["chan"], mesh.shape["beam"])
    return jax.shard_map(body, mesh=mesh, in_specs=in_specs, out_specs=out_specs, check_vma=False)
```

```python
import functools
import math

import jax
import jax.numpy as jnp
from jax import lax
from jax.experimental import pallas as pl
from jax.experimental.pallas import tpu as pltpu
from jax.sharding import PartitionSpec as P

MESH = pl.DeviceIdType.MESH
LANES = 128
ROWS = 16
STREAMS = 4
SENT = jnp.float32
NT = (((1,), (1,)), ((), ()))


def cos_sin(phase, period):
    quarter = period // 4
    turn = (phase + quarter // 2) >> (quarter.bit_length() - 1)
    angle = (phase - turn * quarter).astype(jnp.float32) * (2.0 * math.pi / period)
    square = angle * angle
    sine = angle * (1 + square * (-1 / 6 + square * (1 / 120 + square * (-1 / 5040 + square / 362880))))
    cosine = 1 + square * (
        -1 / 2 + square * (1 / 24 + square * (-1 / 720 + square * (1 / 40320 - square / 3628800)))
    )
    turn = turn & 3
    swap = (turn & 1) == 1
    first = jnp.where(swap, sine, cosine)
    second = jnp.where(swap, cosine, sine)
    cos_value = jnp.where((turn == 1) | (turn == 2), -first, first)
    sin_value = jnp.where(turn >= 2, -second, second)
    return cos_value, sin_value


def flip(index, mask, count):
    if count & (count - 1):
        return lax.rem(index + mask, count)
    result, weight = 0, 1
    while weight < count:
        result = result + (index // weight + mask // weight) % 2 * weight
        weight *= 2
    return result


def loop(count, body):
    if count <= 8:
        for step in range(count):
            body(step)
    else:
        lax.fori_loop(0, count, lambda step, carry: (body(step), carry)[1], 0)


def kernel(
    n_chan, n_beam,
    signals_hbm, weights_hbm, group_ref, out_ref,
    signals, weights, twiddle, part, from_pair, from_far, spectrum, group_rows, formed, arrived,
    load_sem, pair_send, pair_recv, far_send, far_recv, spec_send, spec_recv, form_send, form_recv,
):
    chan, beam = lax.axis_index("chan"), lax.axis_index("beam")
    core = lax.rem(beam, 2)
    far_count = n_beam // 2 - 1
    partner = beam + 1 - 2 * core
    fars = [lax.rem(beam + 2 * (s + 1), n_beam) for s in range(far_count)]

    barrier = pltpu.get_barrier_semaphore()
    for other in [partner] + fars:
        pl.semaphore_signal(barrier, inc=1, device_id={"beam": other}, device_id_type=MESH)

    def greet(step):
        other = flip(chan, n_chan - 1 - step, n_chan)
        pl.semaphore_signal(barrier, inc=1, device_id={"chan": other}, device_id_type=MESH)

    loop(n_chan - 1, greet)

    load_signals = pltpu.make_async_copy(signals_hbm, signals, load_sem.at[0])
    load_weights = pltpu.make_async_copy(weights_hbm, weights, load_sem.at[1])
    load_signals.start()
    load_weights.start()

    bins, samples = part.shape[1], signals.shape[1]
    block = twiddle.shape[1]
    blocks = bins // block
    total = samples * n_beam
    bin_dev = bins // n_chan
    per_block = block // bin_dev
    sets, _, beams, channels = weights.shape
    scale = 1.0 / math.sqrt(total)

    def block_at(step):
        return pl.multiple_of(flip(chan // per_block, blocks - 1 - step, blocks) * block, block)

    def target_of(step):
        return flip(chan, n_chan - 1 - step, n_chan)

    def rows_of(target):
        return pl.ds(pl.multiple_of(target * bin_dev, bin_dev), bin_dev)

    def make_twiddle(start):
        def rows(row, carry):
            base = pl.multiple_of(row * ROWS, ROWS)
            frequency = start + base + 1 + lax.broadcasted_iota(jnp.int32, (ROWS, LANES), 0)
            lane = lax.broadcasted_iota(jnp.int32, (ROWS, LANES), 1)
            cosine, sine = cos_sin((frequency * (beam * samples + lane)) & (total - 1), total)
            stride = STREAMS * LANES
            turns = [(cosine, sine)]
            cos_one, sin_one = cos_sin((frequency * LANES) & (total - 1), total)
            cos_turn, sin_turn = cos_one, sin_one
            doubled = 1
            while doubled < STREAMS:
                turns += [(c * cos_turn - s * sin_turn, s * cos_turn + c * sin_turn) for c, s in turns]
                cos_turn, sin_turn = cos_turn * cos_turn - sin_turn * sin_turn, 2 * cos_turn * sin_turn
                doubled *= 2
            for a in range(0, samples, stride):
                for b, (c, s) in enumerate(turns):
                    at = pl.ds(base, ROWS), pl.ds(a + b * LANES, LANES)
                    twiddle[0, at[0], at[1]] = c.astype(jnp.bfloat16)
                    twiddle[1, at[0], at[1]] = (-s).astype(jnp.bfloat16)
                turns = [(c * cos_turn - s * sin_turn, s * cos_turn + c * sin_turn) for c, s in turns]
            return carry

        lax.fori_loop(0, block // ROWS, rows, 0)

    def transform(kind, start):
        part[kind, pl.ds(start, block)] = lax.dot_general(
            twiddle[kind], signals[...], NT, preferred_element_type=jnp.float32
        )

    def pair_copy(step):
        at = pl.ds(block_at(step), block)
        return pltpu.make_async_remote_copy(
            src_ref=part.at[1 - core, at], dst_ref=from_pair.at[at],
            send_sem=pair_send.at[step], recv_sem=pair_recv.at[step],
            device_id={"beam": partner}, device_id_type=MESH,
        )

    def far_copy(step, s):
        at = rows_of(target_of(step))
        return pltpu.make_async_remote_copy(
            src_ref=part.at[core, at], dst_ref=from_far.at[s, at],
            send_sem=far_send.at[s, step], recv_sem=far_recv.at[s, step],
            device_id={"beam": fars[s]}, device_id_type=MESH,
        )

    def spec_copy(kind, step):
        at = rows_of(target_of(step))
        return pltpu.make_async_remote_copy(
            src_ref=spectrum.at[kind, at], dst_ref=spectrum.at[kind, at],
            send_sem=spec_send.at[step], recv_sem=spec_recv.at[step],
            device_id={"beam": partner}, device_id_type=MESH,
        )

    def form_copy(step):
        target = target_of(step)
        return pltpu.make_async_remote_copy(
            src_ref=formed.at[step], dst_ref=arrived.at[step],
            send_sem=form_send.at[step], recv_sem=form_recv.at[step],
            device_id={"chan": target}, device_id_type=MESH,
        )

    def pair_sum(step):
        pair_copy(step).wait_recv()
        for inner in range(per_block):
            chunk = step * per_block + inner
            at = rows_of(target_of(chunk))
            part[core, at] = part[core, at] + from_pair[at]
            for s in range(far_count):
                far_copy(chunk, s).start()

    make_twiddle(block_at(0))
    load_signals.wait()
    transform(1 - core, block_at(0))
    pl.semaphore_wait(barrier, n_beam // 2 + n_chan - 1)
    pair_copy(0).start()
    transform(core, block_at(0))

    def one_block(before):
        start = block_at(before + 1)
        make_twiddle(start)
        pair_sum(before)
        transform(1 - core, start)
        pair_copy(before + 1).start()
        transform(core, start)

    loop(blocks - 1, one_block)
    pair_sum(blocks - 1)

    group = jnp.broadcast_to(group_ref[...].astype(jnp.float32), (LANES, bins))
    group_rows[...] = group.T
    load_weights.wait()

    def far_sum(step):
        at = rows_of(target_of(step))
        value = part[core, at]
        for s in range(far_count):
            far_copy(step, s).wait_recv()
            value = value + from_far[s, at]
        spectrum[core, at] = (value * scale).astype(jnp.bfloat16)
        spec_copy(core, step).start()

    def form(step):
        at = rows_of(target_of(step))
        spec_copy(1 - core, step).wait_recv()
        products = lax.dot_general(
            spectrum[:, at].reshape(2 * bin_dev, channels),
            weights[...].reshape(sets * 2 * beams, channels), NT, preferred_element_type=jnp.float32,
        )
        ids = group_rows[at, :][:, :1]
        real = imag = jnp.zeros((bin_dev, beams), jnp.float32)
        for g in range(sets):
            left = slice(2 * g * beams, (2 * g + 1) * beams)
            right = slice((2 * g + 1) * beams, (2 * g + 2) * beams)
            real = jnp.where(ids == g, products[:bin_dev, left] - products[bin_dev:, right], real)
            imag = jnp.where(ids == g, products[bin_dev:, left] + products[:bin_dev, right], imag)
        return real, imag

    def send_formed(step):
        real, imag = form(step)
        formed[step, 0] = real.astype(formed.dtype)
        formed[step, 1] = imag.astype(formed.dtype)
        form_copy(step).start()

    def one_chunk(before):
        far_sum(before + 1)
        send_formed(before)

    far_sum(0)
    loop(n_chan - 1, one_chunk)
    real, imag = form(n_chan - 1)
    out_ref[:, 0, :] = real
    out_ref[:, 1, :] = imag

    def collect(step):
        form_copy(step).wait_recv()
        out_ref[:, 0, :] = out_ref[:, 0, :] + arrived[step, 0].astype(jnp.float32)
        out_ref[:, 1, :] = out_ref[:, 1, :] + arrived[step, 1].astype(jnp.float32)

    if n_chan <= 8:
        for step in range(n_chan - 1):
            form_copy(step).wait_recv()
            real = real + arrived[step, 0].astype(jnp.float32)
            imag = imag + arrived[step, 1].astype(jnp.float32)
        out_ref[:, 0, :] = real
        out_ref[:, 1, :] = imag
    else:
        loop(n_chan - 1, collect)

    loop(blocks, lambda step: pair_copy(step).wait_send())
    for s in range(far_count):
        loop(n_chan, lambda step: far_copy(step, s).wait_send())
    loop(n_chan, lambda step: spec_copy(core, step).wait_send())
    loop(n_chan - 1, lambda step: form_copy(step).wait_send())


def shards(n_chan, n_beam, signals, weights, bin_group):
    channels, samples = signals.shape
    sets, _, beams, _ = weights.shape
    bins = bin_group.shape[0]
    bin_dev = bins // n_chan
    fars = n_beam // 2 - 1
    block = min(bins, max(256, bin_dev))
    blocks = bins // block
    dma = pltpu.SemaphoreType.DMA
    return pl.pallas_call(
        functools.partial(kernel, n_chan, n_beam),
        out_shape=jax.ShapeDtypeStruct((bin_dev, 2, beams), jnp.float32),
        in_specs=[
            pl.BlockSpec(memory_space=pl.ANY),
            pl.BlockSpec(memory_space=pl.ANY),
            pl.BlockSpec(memory_space=pltpu.VMEM),
        ],
        out_specs=pl.BlockSpec(memory_space=pltpu.VMEM),
        scratch_shapes=[
            pltpu.VMEM(signals.shape, signals.dtype),
            pltpu.VMEM(weights.shape, weights.dtype),
            pltpu.VMEM((2, block, samples), jnp.bfloat16),
            pltpu.VMEM((2, bins, channels), jnp.float32),
            pltpu.VMEM((bins, channels), jnp.float32),
            pltpu.VMEM((fars, bins, channels), jnp.float32),
            pltpu.VMEM((2, bins, channels), jnp.bfloat16),
            pltpu.VMEM((bins, LANES), jnp.float32),
            pltpu.VMEM((n_chan, 2, bin_dev, beams), SENT),
            pltpu.VMEM((n_chan, 2, bin_dev, beams), SENT),
            dma((2,)), dma((blocks,)), dma((blocks,)), dma((fars, n_chan)), dma((fars, n_chan)),
            dma((n_chan,)), dma((n_chan,)), dma((n_chan,)), dma((n_chan,)),
        ],
        compiler_params=pltpu.CompilerParams(
            collective_id=0, has_side_effects=True, vmem_limit_bytes=60 * 1024 * 1024
        ),
        name="beamform",
    )(signals, weights, bin_group.reshape(1, bins))


def solution(mesh):
    in_specs = (P("chan", "beam"), P(None, None, "beam", "chan"), P())
    out_specs = P("chan", None, "beam")
    body = functools.partial(shards, mesh.shape["chan"], mesh.shape["beam"])
    return jax.shard_map(body, mesh=mesh, in_specs=in_specs, out_specs=out_specs, check_vma=False)
```

```python
import functools
import math

import jax
import jax.numpy as jnp
from jax import lax
from jax.experimental import pallas as pl
from jax.experimental.pallas import tpu as pltpu
from jax.sharding import PartitionSpec as P

MESH = pl.DeviceIdType.MESH
LANES = 128
ROWS = 16
STREAMS = 4
PIECES = 4
SENT = jnp.bfloat16
NT = (((1,), (1,)), ((), ()))


def cos_sin(phase, period):
    quarter = period // 4
    turn = (phase + quarter // 2) >> (quarter.bit_length() - 1)
    angle = (phase - turn * quarter).astype(jnp.float32) * (2.0 * math.pi / period)
    square = angle * angle
    sine = angle * (1 + square * (-1 / 6 + square * (1 / 120 + square * (-1 / 5040 + square / 362880))))
    cosine = 1 + square * (
        -1 / 2 + square * (1 / 24 + square * (-1 / 720 + square * (1 / 40320 - square / 3628800)))
    )
    turn = turn & 3
    swap = (turn & 1) == 1
    first = jnp.where(swap, sine, cosine)
    second = jnp.where(swap, cosine, sine)
    cos_value = jnp.where((turn == 1) | (turn == 2), -first, first)
    sin_value = jnp.where(turn >= 2, -second, second)
    return cos_value, sin_value


def flip(index, mask, count):
    if count & (count - 1):
        return lax.rem(index + mask, count)
    result, weight = 0, 1
    while weight < count:
        result = result + (index // weight + mask // weight) % 2 * weight
        weight *= 2
    return result


def loop(count, body):
    if count <= 8:
        for step in range(count):
            body(step)
    else:
        lax.fori_loop(0, count, lambda step, carry: (body(step), carry)[1], 0)


def kernel(
    n_chan, n_beam,
    signals_hbm, weights_hbm, group_ref, out_ref,
    signals, weights, twiddle, part, from_pair, from_far, spectrum, group_rows, formed, arrived,
    load_sem, pair_send, pair_recv, far_send, far_recv, spec_send, spec_recv, form_send, form_recv,
):
    chan, beam = lax.axis_index("chan"), lax.axis_index("beam")
    core = lax.rem(beam, 2)
    far_count = n_beam // 2 - 1
    partner = beam + 1 - 2 * core
    fars = [lax.rem(beam + 2 * (s + 1), n_beam) for s in range(far_count)]

    barrier = pltpu.get_barrier_semaphore()
    for other in [partner] + fars:
        pl.semaphore_signal(barrier, inc=1, device_id={"beam": other}, device_id_type=MESH)

    def greet(step):
        other = flip(chan, n_chan - 1 - step, n_chan)
        pl.semaphore_signal(barrier, inc=1, device_id={"chan": other}, device_id_type=MESH)

    loop(n_chan - 1, greet)

    load_signals = pltpu.make_async_copy(signals_hbm, signals, load_sem.at[0])
    load_weights = pltpu.make_async_copy(weights_hbm, weights, load_sem.at[1])
    load_signals.start()
    load_weights.start()

    bins, samples = part.shape[1], signals.shape[1]
    block = twiddle.shape[1]
    blocks = bins // block
    total = samples * n_beam
    bin_dev = bins // n_chan
    per_block = block // bin_dev
    sets, _, beams, channels = weights.shape
    scale = 1.0 / math.sqrt(total)

    def block_at(step):
        return pl.multiple_of(flip(chan // per_block, blocks - 1 - step, blocks) * block, block)

    def target_of(step):
        return flip(chan, n_chan - 1 - step, n_chan)

    def rows_of(target):
        return pl.ds(pl.multiple_of(target * bin_dev, bin_dev), bin_dev)

    def make_twiddle(start):
        def rows(row, carry):
            base = pl.multiple_of(row * ROWS, ROWS)
            frequency = start + base + 1 + lax.broadcasted_iota(jnp.int32, (ROWS, LANES), 0)
            lane = lax.broadcasted_iota(jnp.int32, (ROWS, LANES), 1)
            cosine, sine = cos_sin((frequency * (beam * samples + lane)) & (total - 1), total)
            stride = STREAMS * LANES
            turns = [(cosine, sine)]
            cos_one, sin_one = cos_sin((frequency * LANES) & (total - 1), total)
            cos_turn, sin_turn = cos_one, sin_one
            doubled = 1
            while doubled < STREAMS:
                turns += [(c * cos_turn - s * sin_turn, s * cos_turn + c * sin_turn) for c, s in turns]
                cos_turn, sin_turn = cos_turn * cos_turn - sin_turn * sin_turn, 2 * cos_turn * sin_turn
                doubled *= 2
            for a in range(0, samples, stride):
                for b, (c, s) in enumerate(turns):
                    at = pl.ds(base, ROWS), pl.ds(a + b * LANES, LANES)
                    twiddle[0, at[0], at[1]] = c.astype(jnp.bfloat16)
                    twiddle[1, at[0], at[1]] = (-s).astype(jnp.bfloat16)
                turns = [(c * cos_turn - s * sin_turn, s * cos_turn + c * sin_turn) for c, s in turns]
            return carry

        lax.fori_loop(0, block // ROWS, rows, 0)

    def transform(kind, start):
        part[kind, pl.ds(start, block)] = lax.dot_general(
            twiddle[kind], signals[...], NT, preferred_element_type=jnp.float32
        )

    def pair_copy(step):
        size = block // PIECES
        inner = flip(chan % per_block // (per_block // PIECES), PIECES - 1 - step % PIECES, PIECES)
        at = pl.ds(pl.multiple_of(block_at(step // PIECES) + inner * size, size), size)
        return pltpu.make_async_remote_copy(
            src_ref=part.at[1 - core, at], dst_ref=from_pair.at[at],
            send_sem=pair_send.at[step], recv_sem=pair_recv.at[step],
            device_id={"beam": partner}, device_id_type=MESH,
        )

    def far_copy(step, s):
        at = rows_of(target_of(step))
        return pltpu.make_async_remote_copy(
            src_ref=part.at[core, at], dst_ref=from_far.at[s, at],
            send_sem=far_send.at[s, step], recv_sem=far_recv.at[s, step],
            device_id={"beam": fars[s]}, device_id_type=MESH,
        )

    def spec_copy(kind, step):
        at = rows_of(target_of(step))
        return pltpu.make_async_remote_copy(
            src_ref=spectrum.at[kind, at], dst_ref=spectrum.at[kind, at],
            send_sem=spec_send.at[step], recv_sem=spec_recv.at[step],
            device_id={"beam": partner}, device_id_type=MESH,
        )

    def form_copy(step):
        target = target_of(step)
        return pltpu.make_async_remote_copy(
            src_ref=formed.at[step], dst_ref=arrived.at[step],
            send_sem=form_send.at[step], recv_sem=form_recv.at[step],
            device_id={"chan": target}, device_id_type=MESH,
        )

    def pair_sum(step):
        for inner in range(per_block):
            if inner % (per_block // PIECES) == 0:
                pair_copy(step * PIECES + inner // (per_block // PIECES)).wait_recv()
            chunk = step * per_block + inner
            at = rows_of(target_of(chunk))
            part[core, at] = part[core, at] + from_pair[at]
            for s in range(far_count):
                far_copy(chunk, s).start()

    make_twiddle(block_at(0))
    load_signals.wait()
    transform(1 - core, block_at(0))
    pl.semaphore_wait(barrier, n_beam // 2 + n_chan - 1)
    for piece in range(PIECES):
        pair_copy(piece).start()
    transform(core, block_at(0))

    def one_block(before):
        start = block_at(before + 1)
        make_twiddle(start)
        pair_sum(before)
        transform(1 - core, start)
        for piece in range(PIECES):
            pair_copy((before + 1) * PIECES + piece).start()
        transform(core, start)

    loop(blocks - 1, one_block)
    pair_sum(blocks - 1)

    group = jnp.broadcast_to(group_ref[...].astype(jnp.float32), (LANES, bins))
    group_rows[...] = group.T
    load_weights.wait()

    def far_sum(step):
        at = rows_of(target_of(step))
        value = part[core, at]
        for s in range(far_count):
            far_copy(step, s).wait_recv()
            value = value + from_far[s, at]
        spectrum[core, at] = (value * scale).astype(jnp.bfloat16)
        spec_copy(core, step).start()

    def form(step):
        at = rows_of(target_of(step))
        spec_copy(1 - core, step).wait_recv()
        products = lax.dot_general(
            spectrum[:, at].reshape(2 * bin_dev, channels),
            weights[...].reshape(sets * 2 * beams, channels), NT, preferred_element_type=jnp.float32,
        )
        ids = group_rows[at, :][:, :1]
        real = imag = jnp.zeros((bin_dev, beams), jnp.float32)
        for g in range(sets):
            left = slice(2 * g * beams, (2 * g + 1) * beams)
            right = slice((2 * g + 1) * beams, (2 * g + 2) * beams)
            real = jnp.where(ids == g, products[:bin_dev, left] - products[bin_dev:, right], real)
            imag = jnp.where(ids == g, products[bin_dev:, left] + products[:bin_dev, right], imag)
        return real, imag

    def send_formed(step):
        real, imag = form(step)
        formed[step, 0] = real.astype(formed.dtype)
        formed[step, 1] = imag.astype(formed.dtype)
        form_copy(step).start()

    def one_chunk(before):
        far_sum(before + 1)
        send_formed(before)

    far_sum(0)
    loop(n_chan - 1, one_chunk)
    real, imag = form(n_chan - 1)
    real_rows, imag_rows = pl.ds(0, bin_dev, stride=2), pl.ds(1, bin_dev, stride=2)

    def collect(step, value):
        form_copy(step).wait_recv()
        return value[0] + arrived[step, 0].astype(jnp.float32), value[1] + arrived[step, 1].astype(jnp.float32)

    if n_chan <= 8:
        for step in range(n_chan - 1):
            real, imag = collect(step, (real, imag))
    else:
        real, imag = lax.fori_loop(0, n_chan - 1, collect, (real, imag))
    out_ref[real_rows, :] = real
    out_ref[imag_rows, :] = imag

    loop(blocks * PIECES, lambda step: pair_copy(step).wait_send())
    for s in range(far_count):
        loop(n_chan, lambda step: far_copy(step, s).wait_send())
    loop(n_chan, lambda step: spec_copy(core, step).wait_send())
    loop(n_chan - 1, lambda step: form_copy(step).wait_send())


def shards(n_chan, n_beam, signals, weights, bin_group):
    channels, samples = signals.shape
    sets, _, beams, _ = weights.shape
    bins = bin_group.shape[0]
    bin_dev = bins // n_chan
    fars = n_beam // 2 - 1
    block = min(bins, max(256, bin_dev))
    blocks = bins // block
    dma = pltpu.SemaphoreType.DMA
    return pl.pallas_call(
        functools.partial(kernel, n_chan, n_beam),
        out_shape=jax.ShapeDtypeStruct((2 * bin_dev, beams), jnp.float32),
        in_specs=[
            pl.BlockSpec(memory_space=pl.ANY),
            pl.BlockSpec(memory_space=pl.ANY),
            pl.BlockSpec(memory_space=pltpu.VMEM),
        ],
        out_specs=pl.BlockSpec(memory_space=pltpu.VMEM),
        scratch_shapes=[
            pltpu.VMEM(signals.shape, signals.dtype),
            pltpu.VMEM(weights.shape, weights.dtype),
            pltpu.VMEM((2, block, samples), jnp.bfloat16),
            pltpu.VMEM((2, bins, channels), jnp.float32),
            pltpu.VMEM((bins, channels), jnp.float32),
            pltpu.VMEM((fars, bins, channels), jnp.float32),
            pltpu.VMEM((2, bins, channels), jnp.bfloat16),
            pltpu.VMEM((bins, LANES), jnp.float32),
            pltpu.VMEM((n_chan, 2, bin_dev, beams), SENT),
            pltpu.VMEM((n_chan, 2, bin_dev, beams), SENT),
            dma((2,)), dma((blocks * PIECES,)), dma((blocks * PIECES,)), dma((fars, n_chan)), dma((fars, n_chan)),
            dma((n_chan,)), dma((n_chan,)), dma((n_chan,)), dma((n_chan,)),
        ],
        compiler_params=pltpu.CompilerParams(
            collective_id=0, has_side_effects=True, vmem_limit_bytes=60 * 1024 * 1024
        ),
        name="beamform",
    )(signals, weights, bin_group.reshape(1, bins)).reshape(bin_dev, 2, beams)


def solution(mesh):
    in_specs = (P("chan", "beam"), P(None, None, "beam", "chan"), P())
    out_specs = P("chan", None, "beam")
    body = functools.partial(shards, mesh.shape["chan"], mesh.shape["beam"])
    return jax.shard_map(body, mesh=mesh, in_specs=in_specs, out_specs=out_specs, check_vma=False)
```

```python
import functools
import math

import jax
import jax.numpy as jnp
from jax import lax
from jax.experimental import pallas as pl
from jax.experimental.pallas import tpu as pltpu
from jax.sharding import PartitionSpec as P

MESH = pl.DeviceIdType.MESH
LANES = 128
ROWS = 16
STREAMS = 4
PIECES = 4
SENT = jnp.bfloat16
NT = (((1,), (1,)), ((), ()))


def cos_sin(phase, period):
    quarter = period // 4
    turn = (phase + quarter // 2) >> (quarter.bit_length() - 1)
    angle = (phase - turn * quarter).astype(jnp.float32) * (2.0 * math.pi / period)
    square = angle * angle
    sine = angle * (1 + square * (-1 / 6 + square * (1 / 120 + square * (-1 / 5040 + square / 362880))))
    cosine = 1 + square * (
        -1 / 2 + square * (1 / 24 + square * (-1 / 720 + square * (1 / 40320 - square / 3628800)))
    )
    turn = turn & 3
    swap = (turn & 1) == 1
    first = jnp.where(swap, sine, cosine)
    second = jnp.where(swap, cosine, sine)
    cos_value = jnp.where((turn == 1) | (turn == 2), -first, first)
    sin_value = jnp.where(turn >= 2, -second, second)
    return cos_value, sin_value


def flip(index, mask, count):
    if count & (count - 1):
        return lax.rem(index + mask, count)
    result, weight = 0, 1
    while weight < count:
        result = result + (index // weight + mask // weight) % 2 * weight
        weight *= 2
    return result


def loop(count, body):
    if count <= 8:
        for step in range(count):
            body(step)
    else:
        lax.fori_loop(0, count, lambda step, carry: (body(step), carry)[1], 0)


def kernel(
    n_chan, n_beam,
    signals_hbm, weights_hbm, group_ref, out_ref,
    signals, weights, twiddle, part, from_pair, from_far, spectrum, group_rows, formed, arrived,
    load_sem, pair_send, pair_recv, far_send, far_recv, spec_send, spec_recv, form_send, form_recv,
):
    chan, beam = lax.axis_index("chan"), lax.axis_index("beam")
    core = lax.rem(beam, 2)
    far_count = n_beam // 2 - 1
    partner = beam + 1 - 2 * core
    fars = [lax.rem(beam + 2 * (s + 1), n_beam) for s in range(far_count)]

    barrier = pltpu.get_barrier_semaphore()
    for other in [partner] + fars:
        pl.semaphore_signal(barrier, inc=1, device_id={"beam": other}, device_id_type=MESH)

    def greet(step):
        other = flip(chan, n_chan - 1 - step, n_chan)
        pl.semaphore_signal(barrier, inc=1, device_id={"chan": other}, device_id_type=MESH)

    loop(n_chan - 1, greet)

    load_signals = pltpu.make_async_copy(signals_hbm, signals, load_sem.at[0])
    load_weights = pltpu.make_async_copy(weights_hbm, weights, load_sem.at[1])
    load_signals.start()
    load_weights.start()

    bins, samples = part.shape[1], signals.shape[1]
    block = twiddle.shape[1]
    blocks = bins // block
    total = samples * n_beam
    bin_dev = bins // n_chan
    per_block = block // bin_dev
    sets, _, beams, channels = weights.shape
    scale = 1.0 / math.sqrt(total)

    def block_at(step):
        return pl.multiple_of(flip(chan // per_block, blocks - 1 - step, blocks) * block, block)

    def target_of(step):
        return flip(chan, n_chan - 1 - step, n_chan)

    def rows_of(target):
        return pl.ds(pl.multiple_of(target * bin_dev, bin_dev), bin_dev)

    def make_twiddle(start):
        def rows(row, carry):
            base = pl.multiple_of(row * ROWS, ROWS)
            frequency = start + base + 1 + lax.broadcasted_iota(jnp.int32, (ROWS, LANES), 0)
            lane = lax.broadcasted_iota(jnp.int32, (ROWS, LANES), 1)
            cosine, sine = cos_sin((frequency * (beam * samples + lane)) & (total - 1), total)
            stride = STREAMS * LANES
            turns = [(cosine, sine)]
            cos_one, sin_one = cos_sin((frequency * LANES) & (total - 1), total)
            cos_turn, sin_turn = cos_one, sin_one
            doubled = 1
            while doubled < STREAMS:
                turns += [(c * cos_turn - s * sin_turn, s * cos_turn + c * sin_turn) for c, s in turns]
                cos_turn, sin_turn = cos_turn * cos_turn - sin_turn * sin_turn, 2 * cos_turn * sin_turn
                doubled *= 2
            for a in range(0, samples, stride):
                for b, (c, s) in enumerate(turns):
                    at = pl.ds(base, ROWS), pl.ds(a + b * LANES, LANES)
                    twiddle[0, at[0], at[1]] = c.astype(jnp.bfloat16)
                    twiddle[1, at[0], at[1]] = (-s).astype(jnp.bfloat16)
                turns = [(c * cos_turn - s * sin_turn, s * cos_turn + c * sin_turn) for c, s in turns]
            return carry

        lax.fori_loop(0, block // ROWS, rows, 0)

    def transform(kind, start):
        part[kind, pl.ds(start, block)] = lax.dot_general(
            twiddle[kind], signals[...], NT, preferred_element_type=jnp.float32
        )

    def pair_copy(step):
        size = block // PIECES
        inner = flip(chan % per_block // (per_block // PIECES), PIECES - 1 - step % PIECES, PIECES)
        at = pl.ds(pl.multiple_of(block_at(step // PIECES) + inner * size, size), size)
        return pltpu.make_async_remote_copy(
            src_ref=part.at[1 - core, at], dst_ref=from_pair.at[at],
            send_sem=pair_send.at[step], recv_sem=pair_recv.at[step],
            device_id={"beam": partner}, device_id_type=MESH,
        )

    def far_copy(step, s):
        at = rows_of(target_of(step))
        return pltpu.make_async_remote_copy(
            src_ref=part.at[core, at], dst_ref=from_far.at[s, at],
            send_sem=far_send.at[s, step], recv_sem=far_recv.at[s, step],
            device_id={"beam": fars[s]}, device_id_type=MESH,
        )

    def spec_copy(kind, step):
        at = rows_of(target_of(step))
        return pltpu.make_async_remote_copy(
            src_ref=spectrum.at[kind, at], dst_ref=spectrum.at[kind, at],
            send_sem=spec_send.at[step], recv_sem=spec_recv.at[step],
            device_id={"beam": partner}, device_id_type=MESH,
        )

    def form_copy(step):
        target = target_of(step)
        return pltpu.make_async_remote_copy(
            src_ref=formed.at[step], dst_ref=arrived.at[step],
            send_sem=form_send.at[step], recv_sem=form_recv.at[step],
            device_id={"chan": target}, device_id_type=MESH,
        )

    def pair_sum(step):
        for inner in range(per_block):
            if inner % (per_block // PIECES) == 0:
                pair_copy(step * PIECES + inner // (per_block // PIECES)).wait_recv()
            chunk = step * per_block + inner
            at = rows_of(target_of(chunk))
            part[core, at] = part[core, at] + from_pair[at]
            for s in range(far_count):
                far_copy(chunk, s).start()

    make_twiddle(block_at(0))
    load_signals.wait()
    transform(1 - core, block_at(0))
    pl.semaphore_wait(barrier, n_beam // 2 + n_chan - 1)
    for piece in range(PIECES):
        pair_copy(piece).start()
    transform(core, block_at(0))

    def one_block(before):
        start = block_at(before + 1)
        make_twiddle(start)
        pair_sum(before)
        transform(1 - core, start)
        for piece in range(PIECES):
            pair_copy((before + 1) * PIECES + piece).start()
        transform(core, start)

    loop(blocks - 1, one_block)
    pair_sum(blocks - 1)

    group = jnp.broadcast_to(group_ref[...].astype(jnp.float32), (LANES, bins))
    group_rows[...] = group.T
    load_weights.wait()

    def far_sum(step):
        at = rows_of(target_of(step))
        value = part[core, at]
        for s in range(far_count):
            far_copy(step, s).wait_recv()
            value = value + from_far[s, at]
        spectrum[core, at] = (value * scale).astype(jnp.bfloat16)
        spec_copy(core, step).start()

    def form(step):
        at = rows_of(target_of(step))
        spec_copy(1 - core, step).wait_recv()
        products = lax.dot_general(
            spectrum[:, at].reshape(2 * bin_dev, channels),
            weights[...].reshape(sets * 2 * beams, channels), NT, preferred_element_type=jnp.float32,
        )
        ids = group_rows[at, :][:, :1]
        real = imag = jnp.zeros((bin_dev, beams), jnp.float32)
        for g in range(sets):
            left = slice(2 * g * beams, (2 * g + 1) * beams)
            right = slice((2 * g + 1) * beams, (2 * g + 2) * beams)
            real = jnp.where(ids == g, products[:bin_dev, left] - products[bin_dev:, right], real)
            imag = jnp.where(ids == g, products[bin_dev:, left] + products[:bin_dev, right], imag)
        return real, imag

    def send_formed(step):
        real, imag = form(step)
        formed[step, 0] = real.astype(formed.dtype)
        formed[step, 1] = imag.astype(formed.dtype)
        form_copy(step).start()

    def one_chunk(before):
        far_sum(before + 1)
        send_formed(before)

    far_sum(0)
    loop(n_chan - 1, one_chunk)
    real_rows, imag_rows = pl.ds(0, bin_dev, stride=2), pl.ds(1, bin_dev, stride=2)

    def collect(step, value):
        form_copy(step).wait_recv()
        return value[0] + arrived[step, 0].astype(jnp.float32), value[1] + arrived[step, 1].astype(jnp.float32)

    early = n_chan // 2
    value = (jnp.zeros((bin_dev, beams), jnp.float32),) * 2
    if n_chan <= 8:
        for step in range(early):
            value = collect(step, value)
    else:
        value = lax.fori_loop(0, early, collect, value)
    real, imag = form(n_chan - 1)
    real, imag = real + value[0], imag + value[1]
    if n_chan <= 8:
        for step in range(early, n_chan - 1):
            real, imag = collect(step, (real, imag))
    else:
        real, imag = lax.fori_loop(early, n_chan - 1, collect, (real, imag))
    out_ref[real_rows, :] = real
    out_ref[imag_rows, :] = imag

    loop(blocks * PIECES, lambda step: pair_copy(step).wait_send())
    for s in range(far_count):
        loop(n_chan, lambda step: far_copy(step, s).wait_send())
    loop(n_chan, lambda step: spec_copy(core, step).wait_send())
    loop(n_chan - 1, lambda step: form_copy(step).wait_send())


def shards(n_chan, n_beam, signals, weights, bin_group):
    channels, samples = signals.shape
    sets, _, beams, _ = weights.shape
    bins = bin_group.shape[0]
    bin_dev = bins // n_chan
    fars = n_beam // 2 - 1
    block = min(bins, max(256, bin_dev))
    blocks = bins // block
    dma = pltpu.SemaphoreType.DMA
    return pl.pallas_call(
        functools.partial(kernel, n_chan, n_beam),
        out_shape=jax.ShapeDtypeStruct((2 * bin_dev, beams), jnp.float32),
        in_specs=[
            pl.BlockSpec(memory_space=pl.ANY),
            pl.BlockSpec(memory_space=pl.ANY),
            pl.BlockSpec(memory_space=pltpu.VMEM),
        ],
        out_specs=pl.BlockSpec(memory_space=pltpu.VMEM),
        scratch_shapes=[
            pltpu.VMEM(signals.shape, signals.dtype),
            pltpu.VMEM(weights.shape, weights.dtype),
            pltpu.VMEM((2, block, samples), jnp.bfloat16),
            pltpu.VMEM((2, bins, channels), jnp.float32),
            pltpu.VMEM((bins, channels), jnp.float32),
            pltpu.VMEM((fars, bins, channels), jnp.float32),
            pltpu.VMEM((2, bins, channels), jnp.bfloat16),
            pltpu.VMEM((bins, LANES), jnp.float32),
            pltpu.VMEM((n_chan, 2, bin_dev, beams), SENT),
            pltpu.VMEM((n_chan, 2, bin_dev, beams), SENT),
            dma((2,)), dma((blocks * PIECES,)), dma((blocks * PIECES,)), dma((fars, n_chan)), dma((fars, n_chan)),
            dma((n_chan,)), dma((n_chan,)), dma((n_chan,)), dma((n_chan,)),
        ],
        compiler_params=pltpu.CompilerParams(
            collective_id=0, has_side_effects=True, vmem_limit_bytes=60 * 1024 * 1024
        ),
        name="beamform",
    )(signals, weights, bin_group.reshape(1, bins)).reshape(bin_dev, 2, beams)


def solution(mesh):
    in_specs = (P("chan", "beam"), P(None, None, "beam", "chan"), P())
    out_specs = P("chan", None, "beam")
    body = functools.partial(shards, mesh.shape["chan"], mesh.shape["beam"])
    return jax.shard_map(body, mesh=mesh, in_specs=in_specs, out_specs=out_specs, check_vma=False)
```
